32 devices in a mesh: col: 8 (over z, x), bin: 4 (over y, core).
Axes of the slice: x: 2, y: 2, z: 4, core: 2. Of those that a mesh axis runs over, the one named last changes fastest.
Arguments:
- slope: float32 [131072], P('bin'), may hold values from -6 to 6
- curvature: float32 [131072], P('bin'), may hold values from -6 to 0
- target_mean: float32 [131072], P('bin'), may hold values from 0.15 to 0.85
- target_var: float32 [131072], P('bin'), may hold values from 0.06 to 0.12
- table: float32 [64, 512], P(None, 'col'), may hold values from -6 to 6
Outputs:
- species_mean: float32 [64, 131072], P('col')
- final_slope: float32 [131072], replicated
The draws below stay inside these ranges and needn't reach their ends.
All inputs are finite; a program needn't handle non-finite values.
Results may differ from the reference program's by a relative error of at most 0.0001.
Values sent between devices are 32-bit elements; how exact they have to be, the bound alone decides.
A program may use at most 64 MiB of HBM per device.

```python
import math
import jax
import jax.numpy as jnp
from jax import lax

CPTS = 512
SPECIES = 64
ITERS = 3
BINS = 131072


def block_levels(rng, shape, split, smallest, top_value):
    def one(axis_at, blocks):
        heights = jax.random.uniform(jax.random.fold_in(jax.random.fold_in(rng, 6), axis_at), (blocks,), jnp.float32, smallest / len(split), top_value / len(split))
        return jnp.repeat(jnp.exp(heights), shape[axis_at] // blocks).reshape((-1,) + (1,) * (len(shape) - axis_at - 1))

    factor_of = one(*split[0])
    for cut in split[1:]:
        factor_of = factor_of * one(*cut)
    return factor_of


def gaussian(key, shape, spread, bound, pieces=(), dtype=jnp.bfloat16):
    level = block_levels(key, shape, pieces, -0.22, 0.18) if pieces else 1.0
    result = jax.random.normal(key, shape, jnp.float32) * spread * level
    return jnp.minimum(jnp.maximum(result, -bound), bound).astype(dtype)


def setup_inputs(seed: int = 0) -> dict:
    key_list = jax.random.split(jax.random.key(seed), 6)
    return {
        "slope": jnp.clip(jax.random.uniform(key_list[0], (BINS,), jnp.float32, -6.0, 6.0) * block_levels(key_list[0], (BINS,), ((0, 4),), -0.4, 0.0), -6.0, 6.0),
        "curvature": jnp.clip(-6.0 + 6.0 * jax.random.uniform(key_list[1], (BINS,), jnp.float32) ** block_levels(key_list[1], (BINS,), ((0, 4),), -0.2, 0.2), -6.0, 0.0),
        "target_mean": jnp.clip(0.15 + 0.70000002 * jax.random.uniform(key_list[2], (BINS,), jnp.float32) ** block_levels(key_list[2], (BINS,), ((0, 4),), -0.2, 0.2), 0.15, 0.85),
        "target_var": jnp.clip(0.06 + 0.06 * jax.random.uniform(key_list[3], (BINS,), jnp.float32) ** block_levels(key_list[3], (BINS,), ((0, 4),), -0.2, 0.2), 0.06, 0.12),
        "table": gaussian(key_list[4], (SPECIES, CPTS), 1.0, 6.0, ((1, 8),), jnp.float32),
    }


def solve_block(items):
    slope, curvature, target_mean, target_var, table = items
    points = ((jnp.arange(CPTS).astype(jnp.float32) + 0.5) / CPTS)[:, None]
    lam = slope
    for step in range(ITERS):
        expo = jnp.exp(lam[None, :] * points + curvature[None, :] * points * points)
        partition = jnp.sum(expo, axis=0)
        moment = jnp.sum(points * expo, axis=0)
        lam = lam + (target_mean - moment / partition) / target_var
    expo = jnp.exp(lam[None, :] * points + curvature[None, :] * points * points)
    total = jnp.sum(expo, axis=0)
    weights = expo / total[None, :]
    values = jnp.dot(table, weights, precision=lax.Precision.HIGHEST, preferred_element_type=jnp.float32)
    return values, lam


def reference(slope, curvature, target_mean, target_var, table):
    block = math.gcd(BINS, 4096)
    count = BINS // block

    def one(items):
        return solve_block((items[0], items[1], items[2], items[3], table))

    stacked = (slope.reshape(count, block), curvature.reshape(count, block),
               target_mean.reshape(count, block), target_var.reshape(count, block))
    values, lam = lax.map(one, stacked)
    species_mean = jnp.transpose(values, (1, 0, 2)).reshape(SPECIES, BINS)
    return species_mean, lam.reshape(BINS)
```

```python
import functools
import math
import jax
import jax.numpy as jnp
from jax import lax
from jax.experimental import pallas as pl
from jax.experimental.pallas import tpu as pltpu
from jax.sharding import PartitionSpec as P

ITERS = 3
LANES = 128
LOG2E = math.log2(math.e)
MESH = pl.DeviceIdType.MESH
GROUP = 16


def kernel(
    cols, bins, total_pts, rows,
    slope_ref, curve_ref, mean_ref, var_ref, placed_ref,
    out_ref, lam_ref,
    tab, lhs, species,
    bar_unused, tsend, trecv, csend, crecv, ssend, srecv, lsend, lrecv, osem,
):
    del bar_unused
    col = lax.axis_index("col")
    me = lax.axis_index("bin")
    core = lax.rem(me, 2)
    partner = me + 1 - 2 * core
    chips = bins // 2
    width = slope_ref.shape[1] * LANES

    def other_col(i):
        return lax.rem(col + i, cols)

    def other_chip(i):
        return lax.rem(me + 2 * i, bins)

    barrier = pltpu.get_barrier_semaphore()

    @pl.loop(1, cols)
    def _(i):
        pl.semaphore_signal(barrier, inc=1, device_id=(other_col(i), me), device_id_type=MESH)

    for i in range(1, chips):
        pl.semaphore_signal(barrier, inc=1, device_id=(col, other_chip(i)), device_id_type=MESH)
    pl.semaphore_signal(barrier, inc=1, device_id=(col, partner), device_id_type=MESH)

    curve2 = curve_ref[col] * LOG2E
    target = mean_ref[col]
    var = var_ref[col]
    lam = slope_ref[col]

    def newton(lam):
        lam2 = lam * LOG2E

        def body(g, carry):
            part, mom = carry
            for i in range(GROUP):
                c = ((g * GROUP + i).astype(jnp.float32) + 0.5) * (1.0 / total_pts)
                e = jnp.exp2(c * (lam2 + curve2 * c))
                part = part + e
                mom = mom + c * e
            return part, mom

        zero = jnp.zeros_like(lam)
        part, mom = lax.fori_loop(0, total_pts // GROUP, body, (zero, zero))
        return lam + (target - mom / part) / var

    lam = newton(lam)

    pl.semaphore_wait(barrier, cols - 1 + chips)

    def table_copy(i):
        to = other_col(i)
        return pltpu.make_async_remote_copy(
            src_ref=placed_ref.at[to], dst_ref=tab.at[i],
            send_sem=tsend.at[i], recv_sem=trecv.at[i],
            device_id=(to, me), device_id_type=MESH,
        )

    @pl.loop(1, cols)
    def _(i):
        table_copy(i).start()

    for step in range(1, ITERS):
        lam = newton(lam)
    lam_ref[me, col] = lam

    def lam_copy(i):
        to = other_col(i)
        return pltpu.make_async_remote_copy(
            src_ref=lam_ref.at[me, col], dst_ref=lam_ref.at[me, col],
            send_sem=csend.at[i], recv_sem=crecv.at[cols - i],
            device_id=(to, me), device_id_type=MESH,
        )

    def lam_arrival(s):
        src = other_col(s)
        return pltpu.make_async_remote_copy(
            src_ref=lam_ref.at[me, src], dst_ref=lam_ref.at[me, src],
            send_sem=csend.at[s], recv_sem=crecv.at[s],
            device_id=(src, me), device_id_type=MESH,
        )

    @pl.loop(1, cols)
    def _(i):
        lam_copy(i).start()

    @pl.loop(1, cols)
    def _(i):
        table_copy(i).wait()

    full = placed_ref[col]
    full = lax.fori_loop(1, cols, lambda i, acc: acc + tab[i], full)
    high = full.astype(jnp.bfloat16).astype(jnp.float32)
    low = full - high
    pad = full.shape[0]
    ones = jnp.ones((pad, total_pts), jnp.float32)
    lhs[...] = jnp.concatenate([high, low, ones, jnp.zeros_like(ones)], axis=0).astype(jnp.bfloat16)

    def species_copy(n, b, j, dest):
        return pltpu.make_async_remote_copy(
            src_ref=species.at[b, j], dst_ref=species.at[b, j],
            send_sem=ssend.at[n, j], recv_sem=srecv.at[b, j],
            device_id=(col, dest), device_id_type=MESH,
        )

    def slope_copy(n, b, j, dest):
        return pltpu.make_async_remote_copy(
            src_ref=lam_ref.at[b, j], dst_ref=lam_ref.at[b, j],
            send_sem=lsend.at[n, j], recv_sem=lrecv.at[b, j],
            device_id=(col, dest), device_id_type=MESH,
        )

    def write_out(b, j):
        start = pl.multiple_of((b * cols + j) * width, LANES)
        return pltpu.make_async_copy(
            species.at[b, j], out_ref.at[:, pl.ds(start, width)], osem.at[b, j]
        )

    half = min(256, total_pts)

    def compute(j):
        @pl.loop(0, width // (2 * LANES))
        def _(t):
            r = t * 2
            lam_t = jnp.concatenate([lam_ref[me, j, pl.ds(r, 1)], lam_ref[me, j, pl.ds(r + 1, 1)]], axis=1) * LOG2E
            cur_t = jnp.concatenate([curve_ref[j, pl.ds(r, 1)], curve_ref[j, pl.ds(r + 1, 1)]], axis=1) * LOG2E
            acc_h = jnp.zeros((4 * pad, 2 * LANES), jnp.float32)
            for k in range(total_pts // half):
                c = (lax.broadcasted_iota(jnp.int32, (half, 2 * LANES), 0).astype(jnp.float32)
                     + (k * half + 0.5)) * (1.0 / total_pts)
                e = jnp.exp2(c * (lam_t + cur_t * c))
                e_hi = e.astype(jnp.bfloat16)
                e_lo = (e - e_hi.astype(jnp.float32)).astype(jnp.bfloat16)
                w = lhs[:, k * half:(k + 1) * half]
                acc_h = acc_h + jnp.dot(w, e_hi, preferred_element_type=jnp.float32)
                acc_h = acc_h + jnp.dot(w, e_lo, preferred_element_type=jnp.float32)
            total = acc_h[2 * pad:3 * pad]
            value = (acc_h[:pad] + acc_h[pad:2 * pad]) / total
            at = pl.multiple_of(t * 2 * LANES, 2 * LANES)
            species[me, j, :, pl.ds(at, 2 * LANES)] = value[:rows]

    def relay(j):
        for i in range(1, chips):
            b = other_chip(i)
            species_copy(chips + i - 1, b, j, partner).wait_recv()
            species_copy(chips + i - 1, b, j, partner).start()
            write_out(b, j).start()
            slope_copy(chips + i - 1, b, j, partner).wait_recv()
            slope_copy(chips + i - 1, b, j, partner).start()

    def send_own(j):
        for i in range(1, chips):
            species_copy(i, me, j, other_chip(i)).start()
            slope_copy(i, me, j, other_chip(i)).start()
        species_copy(0, me, j, partner).start()
        slope_copy(0, me, j, partner).start()
        write_out(me, j).start()

    @pl.loop(0, cols)
    def _(s):
        j = other_col(s)

        @pl.when(s > 0)
        def _():
            lam_arrival(s).wait_recv()

        compute(j)
        send_own(j)

        @pl.when(s > 1)
        def _():
            relay(other_col(s + cols - 2))

    for s in range(max(cols - 2, 0), cols):
        relay(other_col(s))

    @pl.loop(0, cols)
    def _(s):
        j = other_col(s)
        for i in range(chips):
            b = lax.rem(partner + 2 * i, bins)
            species_copy(0, b, j, partner).wait_recv()
            slope_copy(0, b, j, partner).wait_recv()
            write_out(b, j).start()

    @pl.loop(0, cols)
    def _(s):
        j = other_col(s)
        for n in range(2 * chips - 1):
            species_copy(n, me, j, partner).wait_send()
            slope_copy(n, me, j, partner).wait_send()
        for b in range(bins):
            write_out(b, j).wait()

    @pl.loop(1, cols)
    def _(i):
        lam_copy(i).wait_send()


def per_device(slope, curvature, target_mean, target_var, table):
    cols = lax.axis_size("col")
    bins = lax.axis_size("bin")
    all_species, pts = table.shape
    rows = all_species // cols
    pad = -(-rows // 8) * 8
    total_pts = pts * cols
    per_shard = slope.shape[0]
    sub = per_shard // cols // LANES
    width = sub * LANES

    def blocks(a):
        return a.reshape(cols, sub, LANES)

    placed = jnp.zeros((cols, pad, total_pts), jnp.float32)
    placed = lax.dynamic_update_slice(
        placed, table.reshape(cols, rows, pts), (0, 0, lax.axis_index("col") * pts)
    )
    vmem = pl.BlockSpec(memory_space=pltpu.VMEM)
    chips = bins // 2
    dma = pltpu.SemaphoreType.DMA
    species_mean, lam = pl.pallas_call(
        functools.partial(kernel, cols, bins, total_pts, rows),
        out_shape=(
            jax.ShapeDtypeStruct((rows, per_shard * bins), jnp.float32),
            jax.ShapeDtypeStruct((bins, cols, sub, LANES), jnp.float32),
        ),
        in_specs=[vmem] * 5,
        out_specs=(pl.BlockSpec(memory_space=pl.ANY), vmem),
        scratch_shapes=[
            pltpu.VMEM((cols, pad, total_pts), jnp.float32),
            pltpu.VMEM((4 * pad, total_pts), jnp.bfloat16),
            pltpu.VMEM((bins, cols, rows, width), jnp.float32),
            pltpu.SMEM((1,), jnp.int32),
            dma((cols,)), dma((cols,)),
            dma((cols,)), dma((cols,)),
            dma((2 * chips - 1, cols)), dma((bins, cols)),
            dma((2 * chips - 1, cols)), dma((bins, cols)),
            dma((bins, cols)),
        ],
        compiler_params=pltpu.CompilerParams(collective_id=0, has_side_effects=True, vmem_limit_bytes=48 << 20),
    )(blocks(slope), blocks(curvature), blocks(target_mean), blocks(target_var), placed)
    return species_mean, lam.reshape(-1)


def solution(mesh):
    placed = (P("bin"), P("bin"), P("bin"), P("bin"), P(None, "col"))
    return jax.shard_map(
        per_device, mesh=mesh, in_specs=placed, out_specs=(P("col", None), P()), check_vma=False
    )
```

```python
import functools
import math
import jax
import jax.numpy as jnp
from jax import lax
from jax.experimental import pallas as pl
from jax.experimental.pallas import tpu as pltpu
from jax.sharding import PartitionSpec as P

ITERS = 3
LANES = 128
LOG2E = math.log2(math.e)
MESH = pl.DeviceIdType.MESH
UNROLL = 16
GROUP = 4
PARTS = 4


def kernel(
    cols, bins, total_pts, rows,
    slope_hbm, curve_hbm, mean_hbm, var_hbm, placed_ref,
    out_ref, lam_ref,
    own, curve, tab, lhs, points, stage, species,
    isem, tsend, trecv, ksend, krecv, asend, arecv, bsend, brecv, lsend, lrecv,
    msend, mrecv, ysend, yrecv, psend, precv, osem,
):
    col = lax.axis_index("col")
    me = lax.axis_index("bin")
    core = lax.rem(me, 2)
    partner = me + 1 - 2 * core
    chips = bins // 2
    groups = cols // GROUP
    member = lax.rem(col, GROUP)
    group = col // GROUP
    sub = own.shape[1]
    width = sub * LANES
    part = width // PARTS
    part_rows = sub // PARTS
    pad = placed_ref.shape[1]

    def other_chip(i):
        return lax.rem(me + 2 * i, bins)

    def peer(u, d):
        return lax.rem(group + u, groups) * GROUP + lax.rem(member + d, GROUP)

    def remote(src, dst, send, recv, c, b):
        return pltpu.make_async_remote_copy(
            src_ref=src, dst_ref=dst, send_sem=send, recv_sem=recv,
            device_id=(c, b), device_id_type=MESH,
        )

    barrier = pltpu.get_barrier_semaphore()

    @pl.loop(1, cols)
    def _(i):
        pl.semaphore_signal(barrier, inc=1, device_id=(lax.rem(col + i, cols), me), device_id_type=MESH)

    for i in range(1, chips):
        @pl.loop(0, groups)
        def _(u):
            pl.semaphore_signal(barrier, inc=1, device_id=(peer(u, 0), other_chip(i)), device_id_type=MESH)

    pl.semaphore_signal(barrier, inc=1, device_id=(col, partner), device_id_type=MESH)

    loads = [
        pltpu.make_async_copy(a.at[col], own.at[n], isem.at[n])
        for n, a in enumerate((slope_hbm, mean_hbm, var_hbm))
    ]
    loads.append(pltpu.make_async_copy(curve_hbm, curve.at[me], isem.at[3]))
    for load in loads:
        load.start()
    tab[col] = placed_ref[pl.ds(group * GROUP, GROUP)]
    points[...] = (lax.broadcasted_iota(jnp.int32, points.shape, 0).astype(jnp.float32) + 0.5) * (1.0 / total_pts)
    for load in loads:
        load.wait()

    curve2 = curve[me, col] * LOG2E
    target = own[1]
    var = own[2]
    lam = own[0]

    def newton(lam):
        lam2 = lam * LOG2E

        def body(g, carry):
            total, mom = carry
            for i in range(UNROLL):
                c = ((g * UNROLL + i).astype(jnp.float32) + 0.5) * (1.0 / total_pts)
                e = jnp.exp2(c * (lam2 + curve2 * c))
                total = total + e
                mom = mom + c * e
            return total, mom

        zero = jnp.zeros_like(lam)
        total, mom = lax.fori_loop(0, total_pts // UNROLL, body, (zero, zero))
        return lam + (target - mom / total) / var

    lam = newton(lam)
    pl.semaphore_wait(barrier, cols - 1 + (chips - 1) * groups + 1)

    def table_copy(i):
        to = lax.rem(col + i, cols)
        return remote(placed_ref.at[pl.ds(to // GROUP * GROUP, GROUP)], tab.at[col], tsend.at[i], trecv.at[col], to, me)

    def table_arrival(i):
        src = lax.rem(col + i, cols)
        return remote(tab.at[src], tab.at[src], tsend.at[i], trecv.at[src], src, me)

    def curve_copy(i, u):
        j = peer(u, 0)
        to = other_chip(i)
        return remote(curve.at[me, j], curve.at[me, j], ksend.at[i, u], krecv.at[me // 2, j], col, to)

    def curve_arrival(i, u):
        j = peer(u, 0)
        b = other_chip(i)
        return remote(curve.at[b, j], curve.at[b, j], ksend.at[i, u], krecv.at[b // 2, j], col, b)

    @pl.loop(1, cols)
    def _(i):
        table_copy(i).start()

    for i in range(1, chips):
        @pl.loop(0, groups)
        def _(u):
            curve_copy(i, u).start()

    for step in range(1, ITERS):
        lam = newton(lam)
    lam_ref[me, col] = lam

    def first_copy(i, u):
        return remote(lam_ref.at[me, col], lam_ref.at[me, col], asend.at[i, u], arecv.at[me // 2, col], peer(u, 0), other_chip(i))

    def first_arrival(i, u):
        j = peer(u, 0)
        b = other_chip(i)
        return remote(lam_ref.at[b, j], lam_ref.at[b, j], asend.at[i, u], arecv.at[b // 2, j], j, b)

    @pl.loop(1, groups)
    def _(u):
        first_copy(0, u).start()

    for i in range(1, chips):
        @pl.loop(0, groups)
        def _(u):
            first_copy(i, u).start()

    @pl.loop(1, cols)
    def _(i):
        table_arrival(i).wait_recv()

    per = LANES // (total_pts // cols)
    tiles = []
    for t in range(total_pts // LANES):
        block = tab[t * per]
        for n in range(1, per):
            block = block + tab[t * per + n]
        tiles.append(block.reshape(GROUP * pad, LANES))
    full = jnp.concatenate(tiles, axis=1)
    high = full.astype(jnp.bfloat16).astype(jnp.float32)
    ones = jnp.ones((16, total_pts), jnp.float32)
    lhs[...] = jnp.concatenate([high, full - high, ones], axis=0).astype(jnp.bfloat16)

    span = GROUP * pad

    def lanes(q):
        return pl.ds(pl.multiple_of(q * part, LANES), part)

    def compute(item, b, j, q):
        @pl.loop(0, part_rows // 2)
        def _(t):
            highs, lows = [], []
            for n in range(2):
                r = q * part_rows + t * 2 + n
                lam_t = lam_ref[b, j, pl.ds(r, 1)] * LOG2E
                cur_t = curve[b, j, pl.ds(r, 1)] * LOG2E
                c = points[...]
                e = jnp.exp2(c * (lam_t + cur_t * c))
                e_hi = e.astype(jnp.bfloat16)
                highs.append(e_hi)
                lows.append((e - e_hi.astype(jnp.float32)).astype(jnp.bfloat16))
            acc = jnp.dot(lhs[...], jnp.concatenate(highs, axis=1), preferred_element_type=jnp.float32)
            acc = acc + jnp.dot(lhs[...], jnp.concatenate(lows, axis=1), preferred_element_type=jnp.float32)
            value = (acc[:span] + acc[span:2 * span]) / acc[2 * span:2 * span + 1]
            at = pl.ds(pl.multiple_of(t * 2 * LANES, 2 * LANES), 2 * LANES)
            for n in range(GROUP):
                stage[item, n, :, at] = value[n * pad:n * pad + rows]
            into = pl.ds(pl.multiple_of(q * part + t * 2 * LANES, 2 * LANES), 2 * LANES)
            species[b, j, :, into] = stage[item, member, :, at]

    def member_copy(item, d, b, j, q):
        to = lax.rem(member + d, GROUP)
        return remote(stage.at[item, to], species.at[b, j, :, lanes(q)], msend.at[item, d], mrecv.at[b // 2, j, q], group * GROUP + to, me)

    def member_arrival(b, j, q):
        return remote(species.at[b, j, :, lanes(q)], species.at[b, j, :, lanes(q)], msend.at[0, 0], mrecv.at[b // 2, j, q], lax.rem(col + 1, cols), me)

    def y_copy(i, j, q):
        at = species.at[me, j, :, lanes(q)]
        return remote(at, at, ysend.at[i, j, q], yrecv.at[me // 2, j, q], col, other_chip(i))

    def y_arrival(i, j, q):
        b = other_chip(i)
        at = species.at[b, j, :, lanes(q)]
        return remote(at, at, ysend.at[i, j, q], yrecv.at[b // 2, j, q], col, b)

    def pair_copy(b, j, q):
        at = species.at[b, j, :, lanes(q)]
        return remote(at, at, psend.at[b // 2, j], precv.at[b // 2, j], col, partner)

    def pair_chunk(b, j):
        at = species.at[b, j]
        return remote(at, at, psend.at[b // 2, j], precv.at[b // 2, j], col, partner)

    def write_part(b, j, q):
        start = pl.multiple_of((b * cols + j) * width + q * part, LANES)
        return pltpu.make_async_copy(species.at[b, j, :, lanes(q)], out_ref.at[:, pl.ds(start, part)], osem.at[b, j])

    def write_chunk(b, j):
        start = pl.multiple_of((b * cols + j) * width, LANES)
        return pltpu.make_async_copy(species.at[b, j], out_ref.at[:, pl.ds(start, width)], osem.at[b, j])

    def hand_on(b, j, q):
        pair_copy(b, j, q).start()
        write_part(b, j, q).start()

    singles = groups * (PARTS - 1)

    def single(s):
        return s // (PARTS - 1), 1 + lax.rem(s, PARTS - 1)

    def single_arrivals(s):
        u, q = single(s)
        for d in range(1, GROUP):
            j = peer(u, d)
            member_arrival(me, j, q).wait_recv()
            for i in range(1, chips):
                y_copy(i, j, q).start()
            hand_on(me, j, q)

    @pl.loop(0, singles)
    def _(s):
        u, q = single(s)
        j = peer(u, 0)

        @pl.when(jnp.logical_and(q == 1, u > 0))
        def _():
            first_arrival(0, u).wait_recv()

        compute(s, me, j, q)
        for i in range(1, chips):
            y_copy(i, j, q).start()
        for d in range(1, GROUP):
            member_copy(s, d, me, j, q).start()
        hand_on(me, j, q)

        @pl.when(s > 1)
        def _():
            single_arrivals(s - 2)

    for i in range(1, chips):
        @pl.loop(0, groups)
        def _(u):
            first_arrival(i, u).wait_recv()
            curve_arrival(i, u).wait_recv()

    doubles = groups * chips

    @pl.loop(0, doubles)
    def _(s):
        u = s // chips
        b = lax.rem(me + 2 * lax.rem(s, chips), bins)
        j = peer(u, 0)
        compute(singles + s, b, j, 0)
        for d in range(1, GROUP):
            member_copy(singles + s, d, b, j, 0).start()
        hand_on(b, j, 0)

        @pl.when(s < 2)
        def _():
            single_arrivals(singles - 2 + s)

    def second_copy(d, b, j):
        to = lax.rem(member + d, GROUP)
        return remote(lam_ref.at[b, j], lam_ref.at[b, j], bsend.at[b // 2, j // GROUP, d], brecv.at[b // 2, j], group * GROUP + to, me)

    @pl.loop(0, doubles)
    def _(s):
        b = lax.rem(me + 2 * lax.rem(s, chips), bins)
        for d in range(1, GROUP):
            second_copy(d, b, peer(s // chips, 0)).start()

    @pl.loop(0, doubles)
    def _(s):
        b = lax.rem(me + 2 * lax.rem(s, chips), bins)
        for d in range(1, GROUP):
            j = peer(s // chips, d)
            member_arrival(b, j, 0).wait_recv()
            hand_on(b, j, 0)

    @pl.loop(0, singles)
    def _(s):
        u, q = single(s)
        for d in range(GROUP):
            for i in range(1, chips):
                y_arrival(i, peer(u, d), q).wait_recv()
                hand_on(other_chip(i), peer(u, d), q)

    def lam_pair(b):
        return remote(lam_ref.at[b], lam_ref.at[b], lsend.at[b // 2], lrecv.at[b // 2], col, partner)

    for i in range(chips):
        b = other_chip(i)

        @pl.loop(0, groups)
        def _(u):
            for d in range(1, GROUP):
                second_copy(d, b, peer(u, d)).wait_recv()

        lam_pair(b).start()

    @pl.loop(0, cols)
    def _(j):
        for i in range(chips):
            b = other_chip(i)
            theirs = lax.rem(partner + 2 * i, bins)
            pair_chunk(theirs, j).wait_recv()
            write_chunk(theirs, j).start()

    for i in range(chips):
        lam_pair(other_chip(i)).wait()

    @pl.loop(0, cols)
    def _(j):
        for b in range(bins):
            write_chunk(b, j).wait()
        for i in range(chips):
            pair_chunk(other_chip(i), j).wait_send()
        for i in range(1, chips):
            for q in range(1, PARTS):
                y_copy(i, j, q).wait_send()

    @pl.loop(0, singles + doubles)
    def _(item):
        for d in range(1, GROUP):
            member_copy(item, d, me, col, 0).wait_send()

    @pl.loop(0, doubles)
    def _(s):
        b = lax.rem(me + 2 * lax.rem(s, chips), bins)
        for d in range(1, GROUP):
            second_copy(d, b, peer(s // chips, 0)).wait_send()

    @pl.loop(1, groups)
    def _(u):
        first_copy(0, u).wait_send()

    for i in range(1, chips):
        @pl.loop(0, groups)
        def _(u):
            first_copy(i, u).wait_send()
            curve_copy(i, u).wait_send()

    @pl.loop(1, cols)
    def _(i):
        table_copy(i).wait_send()


def per_device(slope, curvature, target_mean, target_var, table):
    cols = lax.axis_size("col")
    bins = lax.axis_size("bin")
    all_species, pts = table.shape
    rows = all_species // cols
    pad = -(-rows // 8) * 8
    total_pts = pts * cols
    per_shard = slope.shape[0]
    sub = per_shard // cols // LANES
    width = sub * LANES
    chips = bins // 2
    groups = cols // GROUP
    items = groups * (PARTS - 1 + chips)

    def blocks(a):
        return a.reshape(cols, sub, LANES)

    placed = lax.dynamic_update_slice(
        jnp.zeros((cols, pad, LANES), jnp.float32),
        table.reshape(cols, rows, pts),
        (0, 0, lax.axis_index("col") * pts % LANES),
    )
    vmem = pl.BlockSpec(memory_space=pltpu.VMEM)
    hbm = pl.BlockSpec(memory_space=pltpu.HBM)
    dma = pltpu.SemaphoreType.DMA
    species_mean, lam = pl.pallas_call(
        functools.partial(kernel, cols, bins, total_pts, rows),
        out_shape=(
            jax.ShapeDtypeStruct((rows, per_shard * bins), jnp.float32),
            jax.ShapeDtypeStruct((bins, cols, sub, LANES), jnp.float32),
        ),
        in_specs=[hbm] * 4 + [vmem],
        out_specs=(pl.BlockSpec(memory_space=pl.ANY), vmem),
        scratch_shapes=[
            pltpu.VMEM((3, sub, LANES), jnp.float32),
            pltpu.VMEM((bins, cols, sub, LANES), jnp.float32),
            pltpu.VMEM((cols, GROUP, pad, LANES), jnp.float32),
            pltpu.VMEM((2 * GROUP * pad + 16, total_pts), jnp.bfloat16),
            pltpu.VMEM((total_pts, LANES), jnp.float32),
            pltpu.VMEM((items, GROUP, rows, width // PARTS), jnp.float32),
            pltpu.VMEM((bins, cols, rows, width), jnp.float32),
            dma((4,)),
            dma((cols,)), dma((cols,)),
            dma((chips, groups)), dma((chips, cols)),
            dma((chips, groups)), dma((chips, cols)),
            dma((chips, groups, GROUP)), dma((chips, cols)),
            dma((chips,)), dma((chips,)),
            dma((items, GROUP)), dma((chips, cols, PARTS)),
            dma((chips, cols, PARTS)), dma((chips, cols, PARTS)),
            dma((chips, cols)), dma((chips, cols)),
            dma((bins, cols)),
        ],
        compiler_params=pltpu.CompilerParams(collective_id=0, has_side_effects=True, vmem_limit_bytes=40 << 20),
    )(blocks(slope), blocks(curvature), blocks(target_mean), blocks(target_var), placed)
    return species_mean, lam.reshape(-1)


def solution(mesh):
    placed = (P("bin"), P("bin"), P("bin"), P("bin"), P(None, "col"))
    return jax.shard_map(
        per_device, mesh=mesh, in_specs=placed, out_specs=(P("col", None), P()), check_vma=False
    )
```

```python
import functools
import math
import jax
import jax.numpy as jnp
from jax import lax
from jax.experimental import pallas as pl
from jax.experimental.pallas import tpu as pltpu
from jax.sharding import PartitionSpec as P

ITERS = 3
LANES = 128
LOG2E = math.log2(math.e)
MESH = pl.DeviceIdType.MESH
UNROLL = 16
GROUP = 4
PARTS = 4


def kernel(
    cols, bins, total_pts, rows,
    slope_hbm, curve_hbm, mean_hbm, var_hbm, placed_ref,
    out_ref, lam_ref,
    own, curve, tab, lhs, points, stage, species,
    isem, tsend, trecv, ksend, krecv, asend, arecv, bsend, brecv, lsend, lrecv,
    msend, mrecv, ysend, yrecv, psend, precv, osem,
):
    col = lax.axis_index("col")
    me = lax.axis_index("bin")
    core = lax.rem(me, 2)
    partner = me + 1 - 2 * core
    chips = bins // 2
    groups = cols // GROUP
    member = lax.rem(col, GROUP)
    group = col // GROUP
    sub = own.shape[1]
    width = sub * LANES
    part = width // PARTS
    part_rows = sub // PARTS
    pad = placed_ref.shape[1]

    def other_chip(i):
        return lax.rem(me + 2 * i, bins)

    def peer(u, d):
        return lax.rem(group + u, groups) * GROUP + lax.rem(member + d, GROUP)

    def remote(src, dst, send, recv, c, b):
        return pltpu.make_async_remote_copy(
            src_ref=src, dst_ref=dst, send_sem=send, recv_sem=recv,
            device_id=(c, b), device_id_type=MESH,
        )

    barrier = pltpu.get_barrier_semaphore()

    @pl.loop(1, cols)
    def _(i):
        pl.semaphore_signal(barrier, inc=1, device_id=(lax.rem(col + i, cols), me), device_id_type=MESH)

    for i in range(1, chips):
        @pl.loop(0, groups)
        def _(u):
            pl.semaphore_signal(barrier, inc=1, device_id=(peer(u, 0), other_chip(i)), device_id_type=MESH)

    pl.semaphore_signal(barrier, inc=1, device_id=(col, partner), device_id_type=MESH)

    loads = [
        pltpu.make_async_copy(a.at[col], own.at[n], isem.at[n])
        for n, a in enumerate((slope_hbm, mean_hbm, var_hbm))
    ]
    loads.append(pltpu.make_async_copy(curve_hbm, curve.at[me], isem.at[3]))
    for load in loads:
        load.start()
    tab[col] = placed_ref[pl.ds(group * GROUP, GROUP)]
    points[...] = (lax.broadcasted_iota(jnp.int32, points.shape, 0).astype(jnp.float32) + 0.5) * (1.0 / total_pts)
    for load in loads:
        load.wait()

    curve2 = curve[me, col] * LOG2E
    target = own[1]
    var = own[2]
    lam = own[0]

    h = 1.0 / total_pts
    bend = jnp.exp2(curve2 * (2.0 * h * h))

    def newton(lam):
        lam2 = lam * LOG2E

        def body(g, carry):
            total, mom = carry
            c = ((g * UNROLL).astype(jnp.float32) + 0.5) * h
            e = jnp.exp2(c * (lam2 + curve2 * c))
            ratio = jnp.exp2(h * (lam2 + curve2 * (2.0 * c + h)))
            run = e
            runs = e
            for i in range(1, UNROLL):
                e = e * ratio
                if i < UNROLL - 1:
                    ratio = ratio * bend
                run = run + e
                runs = runs + run
            return total + run, mom + (c * run + h * (UNROLL * run - runs))

        zero = jnp.zeros_like(lam)
        total, mom = lax.fori_loop(0, total_pts // UNROLL, body, (zero, zero))
        return lam + (target - mom / total) / var

    lam = newton(lam)
    pl.semaphore_wait(barrier, cols - 1 + (chips - 1) * groups + 1)

    def table_copy(i):
        to = lax.rem(col + i, cols)
        return remote(placed_ref.at[pl.ds(to // GROUP * GROUP, GROUP)], tab.at[col], tsend.at[i], trecv.at[col], to, me)

    def table_arrival(i):
        src = lax.rem(col + i, cols)
        return remote(tab.at[src], tab.at[src], tsend.at[i], trecv.at[src], src, me)

    def curve_copy(i, u):
        j = peer(u, 0)
        to = other_chip(i)
        return remote(curve.at[me, j], curve.at[me, j], ksend.at[i, u], krecv.at[me // 2, j], col, to)

    def curve_arrival(i, u):
        j = peer(u, 0)
        b = other_chip(i)
        return remote(curve.at[b, j], curve.at[b, j], ksend.at[i, u], krecv.at[b // 2, j], col, b)

    @pl.loop(1, cols)
    def _(i):
        table_copy(i).start()

    for i in range(1, chips):
        @pl.loop(0, groups)
        def _(u):
            curve_copy(i, u).start()

    for step in range(1, ITERS):
        lam = newton(lam)
    lam_ref[me, col] = lam

    def first_copy(i, u):
        return remote(lam_ref.at[me, col], lam_ref.at[me, col], asend.at[i, u], arecv.at[me // 2, col], peer(u, 0), other_chip(i))

    def first_arrival(i, u):
        j = peer(u, 0)
        b = other_chip(i)
        return remote(lam_ref.at[b, j], lam_ref.at[b, j], asend.at[i, u], arecv.at[b // 2, j], j, b)

    @pl.loop(1, groups)
    def _(u):
        first_copy(0, u).start()

    for i in range(1, chips):
        @pl.loop(0, groups)
        def _(u):
            first_copy(i, u).start()

    @pl.loop(1, cols)
    def _(i):
        table_arrival(i).wait_recv()

    full = jnp.concatenate(
        [jnp.concatenate([tab[t, n] for n in range(GROUP)], axis=0) for t in range(cols)], axis=1
    )
    high = full.astype(jnp.bfloat16).astype(jnp.float32)
    ones = jnp.ones((16, total_pts), jnp.float32)
    lhs[...] = jnp.concatenate([high, full - high, ones], axis=0).astype(jnp.bfloat16)

    span = GROUP * pad

    def lanes(q):
        return pl.ds(pl.multiple_of(q * part, LANES), part)

    def compute(item, b, j, q):
        @pl.loop(0, part_rows // 2)
        def _(t):
            highs, lows = [], []
            for n in range(2):
                r = q * part_rows + t * 2 + n
                lam_t = lam_ref[b, j, pl.ds(r, 1)] * LOG2E
                cur_t = curve[b, j, pl.ds(r, 1)] * LOG2E
                c = points[...]
                e = jnp.exp2(c * (lam_t + cur_t * c))
                e_hi = e.astype(jnp.bfloat16)
                highs.append(e_hi)
                lows.append((e - e_hi.astype(jnp.float32)).astype(jnp.bfloat16))
            acc = jnp.dot(lhs[...], jnp.concatenate(highs, axis=1), preferred_element_type=jnp.float32)
            acc = acc + jnp.dot(lhs[...], jnp.concatenate(lows, axis=1), preferred_element_type=jnp.float32)
            value = (acc[:span] + acc[span:2 * span]) / acc[2 * span:2 * span + 1]
            at = pl.ds(pl.multiple_of(t * 2 * LANES, 2 * LANES), 2 * LANES)
            for n in range(GROUP):
                stage[item, n, :, at] = value[n * pad:n * pad + rows]
            into = pl.ds(pl.multiple_of(q * part + t * 2 * LANES, 2 * LANES), 2 * LANES)
            species[b, j, :, into] = stage[item, member, :, at]

    def member_copy(item, d, b, j, q):
        to = lax.rem(member + d, GROUP)
        return remote(stage.at[item, to], species.at[b, j, :, lanes(q)], msend.at[item, d], mrecv.at[b // 2, j, q], group * GROUP + to, me)

    def member_arrival(b, j, q):
        return remote(species.at[b, j, :, lanes(q)], species.at[b, j, :, lanes(q)], msend.at[0, 0], mrecv.at[b // 2, j, q], lax.rem(col + 1, cols), me)

    def y_copy(i, j, q):
        at = species.at[me, j, :, lanes(q)]
        return remote(at, at, ysend.at[i, j, q], yrecv.at[me // 2, j, q], col, other_chip(i))

    def y_arrival(i, j, q):
        b = other_chip(i)
        at = species.at[b, j, :, lanes(q)]
        return remote(at, at, ysend.at[i, j, q], yrecv.at[b // 2, j, q], col, b)

    def pair_copy(b, j, q):
        at = species.at[b, j, :, lanes(q)]
        return remote(at, at, psend.at[b // 2, j], precv.at[b // 2, j], col, partner)

    def pair_chunk(b, j):
        at = species.at[b, j]
        return remote(at, at, psend.at[b // 2, j], precv.at[b // 2, j], col, partner)

    def write_part(b, j, q):
        start = pl.multiple_of((b * cols + j) * width + q * part, LANES)
        return pltpu.make_async_copy(species.at[b, j, :, lanes(q)], out_ref.at[:, pl.ds(start, part)], osem.at[b, j])

    def write_chunk(b, j):
        start = pl.multiple_of((b * cols + j) * width, LANES)
        return pltpu.make_async_copy(species.at[b, j], out_ref.at[:, pl.ds(start, width)], osem.at[b, j])

    def hand_on(b, j, q):
        pair_copy(b, j, q).start()
        write_part(b, j, q).start()

    singles = groups * (PARTS - 1)

    def single(s):
        return s // (PARTS - 1), 1 + lax.rem(s, PARTS - 1)

    def single_arrivals(s):
        u, q = single(s)
        for d in range(1, GROUP):
            j = peer(u, d)
            member_arrival(me, j, q).wait_recv()
            for i in range(1, chips):
                y_copy(i, j, q).start()
            hand_on(me, j, q)

    @pl.loop(0, singles)
    def _(s):
        u, q = single(s)
        j = peer(u, 0)

        @pl.when(jnp.logical_and(q == 1, u > 0))
        def _():
            first_arrival(0, u).wait_recv()

        compute(s, me, j, q)
        for i in range(1, chips):
            y_copy(i, j, q).start()
        for d in range(1, GROUP):
            member_copy(s, d, me, j, q).start()
        hand_on(me, j, q)

        @pl.when(s > 1)
        def _():
            single_arrivals(s - 2)

    for i in range(1, chips):
        @pl.loop(0, groups)
        def _(u):
            first_arrival(i, u).wait_recv()
            curve_arrival(i, u).wait_recv()

    doubles = groups * chips

    @pl.loop(0, doubles)
    def _(s):
        u = s // chips
        b = lax.rem(me + 2 * lax.rem(s, chips), bins)
        j = peer(u, 0)
        compute(singles + s, b, j, 0)
        for d in range(1, GROUP):
            member_copy(singles + s, d, b, j, 0).start()
        hand_on(b, j, 0)

        @pl.when(s < 2)
        def _():
            single_arrivals(singles - 2 + s)

    def second_copy(d, b, j):
        to = lax.rem(member + d, GROUP)
        return remote(lam_ref.at[b, j], lam_ref.at[b, j], bsend.at[b // 2, j // GROUP, d], brecv.at[b // 2, j], group * GROUP + to, me)

    @pl.loop(0, doubles)
    def _(s):
        b = lax.rem(me + 2 * lax.rem(s, chips), bins)
        for d in range(1, GROUP):
            second_copy(d, b, peer(s // chips, 0)).start()

    @pl.loop(0, doubles)
    def _(s):
        b = lax.rem(me + 2 * lax.rem(s, chips), bins)
        for d in range(1, GROUP):
            j = peer(s // chips, d)
            member_arrival(b, j, 0).wait_recv()
            hand_on(b, j, 0)

    @pl.loop(0, singles)
    def _(s):
        u, q = single(s)
        for d in range(GROUP):
            for i in range(1, chips):
                y_arrival(i, peer(u, d), q).wait_recv()
                hand_on(other_chip(i), peer(u, d), q)

    def lam_pair(b):
        return remote(lam_ref.at[b], lam_ref.at[b], lsend.at[b // 2], lrecv.at[b // 2], col, partner)

    for i in range(chips):
        b = other_chip(i)

        @pl.loop(0, groups)
        def _(u):
            for d in range(1, GROUP):
                second_copy(d, b, peer(u, d)).wait_recv()

        lam_pair(b).start()

    @pl.loop(0, cols)
    def _(j):
        for i in range(chips):
            b = other_chip(i)
            theirs = lax.rem(partner + 2 * i, bins)
            pair_chunk(theirs, j).wait_recv()
            write_chunk(theirs, j).start()

    for i in range(chips):
        lam_pair(other_chip(i)).wait()

    @pl.loop(0, cols)
    def _(j):
        for b in range(bins):
            write_chunk(b, j).wait()
        for i in range(chips):
            pair_chunk(other_chip(i), j).wait_send()
        for i in range(1, chips):
            for q in range(1, PARTS):
                y_copy(i, j, q).wait_send()

    @pl.loop(0, singles + doubles)
    def _(item):
        for d in range(1, GROUP):
            member_copy(item, d, me, col, 0).wait_send()

    @pl.loop(0, doubles)
    def _(s):
        b = lax.rem(me + 2 * lax.rem(s, chips), bins)
        for d in range(1, GROUP):
            second_copy(d, b, peer(s // chips, 0)).wait_send()

    @pl.loop(1, groups)
    def _(u):
        first_copy(0, u).wait_send()

    for i in range(1, chips):
        @pl.loop(0, groups)
        def _(u):
            first_copy(i, u).wait_send()
            curve_copy(i, u).wait_send()

    @pl.loop(1, cols)
    def _(i):
        table_copy(i).wait_send()


def per_device(slope, curvature, target_mean, target_var, table):
    cols = lax.axis_size("col")
    bins = lax.axis_size("bin")
    all_species, pts = table.shape
    rows = all_species // cols
    pad = rows
    total_pts = pts * cols
    per_shard = slope.shape[0]
    sub = per_shard // cols // LANES
    width = sub * LANES
    chips = bins // 2
    groups = cols // GROUP
    items = groups * (PARTS - 1 + chips)

    def blocks(a):
        return a.reshape(cols, sub, LANES)

    placed = table.reshape(cols, rows, pts)
    vmem = pl.BlockSpec(memory_space=pltpu.VMEM)
    hbm = pl.BlockSpec(memory_space=pltpu.HBM)
    dma = pltpu.SemaphoreType.DMA
    species_mean, lam = pl.pallas_call(
        functools.partial(kernel, cols, bins, total_pts, rows),
        out_shape=(
            jax.ShapeDtypeStruct((rows, per_shard * bins), jnp.float32),
            jax.ShapeDtypeStruct((bins, cols, sub, LANES), jnp.float32),
        ),
        in_specs=[hbm] * 4 + [vmem],
        out_specs=(pl.BlockSpec(memory_space=pl.ANY), vmem),
        scratch_shapes=[
            pltpu.VMEM((3, sub, LANES), jnp.float32),
            pltpu.VMEM((bins, cols, sub, LANES), jnp.float32),
            pltpu.VMEM((cols, GROUP, pad, pts), jnp.float32),
            pltpu.VMEM((2 * GROUP * pad + 16, total_pts), jnp.bfloat16),
            pltpu.VMEM((total_pts, LANES), jnp.float32),
            pltpu.VMEM((items, GROUP, rows, width // PARTS), jnp.float32),
            pltpu.VMEM((bins, cols, rows, width), jnp.float32),
            dma((4,)),
            dma((cols,)), dma((cols,)),
            dma((chips, groups)), dma((chips, cols)),
            dma((chips, groups)), dma((chips, cols)),
            dma((chips, groups, GROUP)), dma((chips, cols)),
            dma((chips,)), dma((chips,)),
            dma((items, GROUP)), dma((chips, cols, PARTS)),
            dma((chips, cols, PARTS)), dma((chips, cols, PARTS)),
            dma((chips, cols)), dma((chips, cols)),
            dma((bins, cols)),
        ],
        compiler_params=pltpu.CompilerParams(collective_id=0, has_side_effects=True, vmem_limit_bytes=40 << 20),
    )(*[
        pltpu.with_memory_space_constraint(a, pltpu.HBM)
        for a in (blocks(slope), blocks(curvature), blocks(target_mean), blocks(target_var))
    ], placed)
    return species_mean, lam.reshape(-1)


def solution(mesh):
    placed = (P("bin"), P("bin"), P("bin"), P("bin"), P(None, "col"))
    return jax.shard_map(
        per_device, mesh=mesh, in_specs=placed, out_specs=(P("col", None), P()), check_vma=False
    )
```

```python
import functools
import math
import jax
import jax.numpy as jnp
from jax import lax
from jax.experimental import pallas as pl
from jax.experimental.pallas import tpu as pltpu
from jax.sharding import PartitionSpec as P

ITERS = 3
LANES = 128
LOG2E = math.log2(math.e)
MESH = pl.DeviceIdType.MESH
UNROLL = 16
GROUP = 4
PARTS = 4


def kernel(
    cols, bins, total_pts, rows,
    slope_hbm, curve_hbm, mean_hbm, var_hbm, placed_ref,
    out_ref, lam_ref,
    own, curve, tab, lhs, points, stage, species,
    isem, tsend, trecv, ksend, krecv, asend, arecv, bsend, brecv, lsend, lrecv,
    msend, mrecv, ysend, yrecv, psend, precv, osem,
):
    col = lax.axis_index("col")
    me = lax.axis_index("bin")
    core = lax.rem(me, 2)
    partner = me + 1 - 2 * core
    chips = bins // 2
    groups = cols // GROUP
    member = lax.rem(col, GROUP)
    group = col // GROUP
    sub = own.shape[1]
    width = sub * LANES
    part = width // PARTS
    part_rows = sub // PARTS
    pad = placed_ref.shape[1]

    def other_chip(i):
        return lax.rem(me + 2 * i, bins)

    def peer(u, d):
        return lax.rem(group + u, groups) * GROUP + lax.rem(member + d, GROUP)

    def remote(src, dst, send, recv, c, b):
        return pltpu.make_async_remote_copy(
            src_ref=src, dst_ref=dst, send_sem=send, recv_sem=recv,
            device_id=(c, b), device_id_type=MESH,
        )

    barrier = pltpu.get_barrier_semaphore()

    @pl.loop(1, cols)
    def _(i):
        pl.semaphore_signal(barrier, inc=1, device_id=(lax.rem(col + i, cols), me), device_id_type=MESH)

    for i in range(1, chips):
        @pl.loop(0, groups)
        def _(u):
            pl.semaphore_signal(barrier, inc=1, device_id=(peer(u, 0), other_chip(i)), device_id_type=MESH)

    pl.semaphore_signal(barrier, inc=1, device_id=(col, partner), device_id_type=MESH)

    loads = [
        pltpu.make_async_copy(a.at[col], own.at[n], isem.at[n])
        for n, a in enumerate((slope_hbm, mean_hbm, var_hbm))
    ]
    loads.append(pltpu.make_async_copy(curve_hbm, curve.at[me], isem.at[3]))
    for load in loads:
        load.start()
    tab[col] = placed_ref[pl.ds(group * GROUP, GROUP)]
    points[...] = (lax.broadcasted_iota(jnp.int32, points.shape, 0).astype(jnp.float32) + 0.5) * (1.0 / total_pts)
    for load in loads:
        load.wait()

    curve2 = curve[me, col] * LOG2E
    target = own[1]
    var = own[2]
    lam = own[0]

    h = 1.0 / total_pts
    bend = jnp.exp2(curve2 * (2.0 * h * h))

    def newton(lam):
        lam2 = lam * LOG2E

        def body(g, carry):
            total, mom = carry
            c = ((g * UNROLL).astype(jnp.float32) + 0.5) * h
            e = jnp.exp2(c * (lam2 + curve2 * c))
            ratio = jnp.exp2(h * (lam2 + curve2 * (2.0 * c + h)))
            run = e
            runs = e
            for i in range(1, UNROLL):
                e = e * ratio
                if i < UNROLL - 1:
                    ratio = ratio * bend
                run = run + e
                runs = runs + run
            return total + run, mom + (c * run + h * (UNROLL * run - runs))

        zero = jnp.zeros_like(lam)
        total, mom = lax.fori_loop(0, total_pts // UNROLL, body, (zero, zero))
        return lam + (target - mom / total) / var

    lam = newton(lam)
    pl.semaphore_wait(barrier, cols - 1 + (chips - 1) * groups + 1)

    def table_copy(i):
        to = lax.rem(col + i, cols)
        return remote(placed_ref.at[pl.ds(to // GROUP * GROUP, GROUP)], tab.at[col], tsend.at[i], trecv.at[col], to, me)

    def table_arrival(i):
        src = lax.rem(col + i, cols)
        return remote(tab.at[src], tab.at[src], tsend.at[i], trecv.at[src], src, me)

    def curve_copy(i, u):
        j = peer(u, 0)
        to = other_chip(i)
        return remote(curve.at[me, j], curve.at[me, j], ksend.at[i, u], krecv.at[me // 2, j], col, to)

    def curve_arrival(i, u):
        j = peer(u, 0)
        b = other_chip(i)
        return remote(curve.at[b, j], curve.at[b, j], ksend.at[i, u], krecv.at[b // 2, j], col, b)

    @pl.loop(1, cols)
    def _(i):
        table_copy(i).start()

    for i in range(1, chips):
        @pl.loop(0, groups)
        def _(u):
            curve_copy(i, u).start()

    for step in range(1, ITERS):
        lam = newton(lam)
    lam_ref[me, col] = lam

    def first_copy(i, u):
        return remote(lam_ref.at[me, col], lam_ref.at[me, col], asend.at[i, u], arecv.at[me // 2, col], peer(u, 0), other_chip(i))

    def first_arrival(i, u):
        j = peer(u, 0)
        b = other_chip(i)
        return remote(lam_ref.at[b, j], lam_ref.at[b, j], asend.at[i, u], arecv.at[b // 2, j], j, b)

    @pl.loop(1, groups)
    def _(u):
        first_copy(0, u).start()

    for i in range(1, chips):
        @pl.loop(0, groups)
        def _(u):
            first_copy(i, u).start()

    @pl.loop(1, cols)
    def _(i):
        table_arrival(i).wait_recv()

    full = jnp.concatenate(
        [jnp.concatenate([tab[t, n] for n in range(GROUP)], axis=0) for t in range(cols)], axis=1
    )
    high = full.astype(jnp.bfloat16).astype(jnp.float32)
    ones = jnp.ones((16, total_pts), jnp.float32)
    lhs[...] = jnp.concatenate([high, full - high, ones], axis=0).astype(jnp.bfloat16)

    span = GROUP * pad

    def lanes(q):
        return pl.ds(pl.multiple_of(q * part, LANES), part)

    def compute(item, b, j, q):
        @pl.loop(0, part_rows // 2)
        def _(t):
            highs, lows = [], []
            for n in range(2):
                r = q * part_rows + t * 2 + n
                lam_t = lam_ref[b, j, pl.ds(r, 1)] * LOG2E
                cur_t = curve[b, j, pl.ds(r, 1)] * LOG2E
                c = points[...]
                e = jnp.exp2(c * (lam_t + cur_t * c))
                e_hi = e.astype(jnp.bfloat16)
                highs.append(e_hi)
                lows.append((e - e_hi.astype(jnp.float32)).astype(jnp.bfloat16))
            acc = jnp.dot(lhs[...], jnp.concatenate(highs, axis=1), preferred_element_type=jnp.float32)
            acc = acc + jnp.dot(lhs[...], jnp.concatenate(lows, axis=1), preferred_element_type=jnp.float32)
            value = (acc[:span] + acc[span:2 * span]) / acc[2 * span:2 * span + 1]
            at = pl.ds(pl.multiple_of(t * 2 * LANES, 2 * LANES), 2 * LANES)
            for n in range(GROUP):
                stage[item, n, :, at] = value[n * pad:n * pad + rows]
            into = pl.ds(pl.multiple_of(q * part + t * 2 * LANES, 2 * LANES), 2 * LANES)
            species[b, j, :, into] = stage[item, member, :, at]

    def member_copy(item, d, b, j, q):
        to = lax.rem(member + d, GROUP)
        return remote(stage.at[item, to], species.at[b, j, :, lanes(q)], msend.at[item, d], mrecv.at[b // 2, j, q], group * GROUP + to, me)

    def member_arrival(b, j, q):
        return remote(species.at[b, j, :, lanes(q)], species.at[b, j, :, lanes(q)], msend.at[0, 0], mrecv.at[b // 2, j, q], lax.rem(col + 1, cols), me)

    def y_copy(i, j, q):
        at = species.at[me, j, :, lanes(q)]
        return remote(at, at, ysend.at[i, j, q], yrecv.at[me // 2, j, q], col, other_chip(i))

    def y_arrival(i, j, q):
        b = other_chip(i)
        at = species.at[b, j, :, lanes(q)]
        return remote(at, at, ysend.at[i, j, q], yrecv.at[b // 2, j, q], col, b)

    def pair_copy(b, j, q):
        at = species.at[b, j, :, lanes(q)]
        return remote(at, at, psend.at[b // 2, j], precv.at[b // 2, j], col, partner)

    def pair_chunk(b, j):
        at = species.at[b, j]
        return remote(at, at, psend.at[b // 2, j], precv.at[b // 2, j], col, partner)

    def write_part(b, j, q):
        start = pl.multiple_of((b * cols + j) * width + q * part, LANES)
        return pltpu.make_async_copy(species.at[b, j, :, lanes(q)], out_ref.at[:, pl.ds(start, part)], osem.at[b, j])

    def write_chunk(b, j):
        start = pl.multiple_of((b * cols + j) * width, LANES)
        return pltpu.make_async_copy(species.at[b, j], out_ref.at[:, pl.ds(start, width)], osem.at[b, j])

    def hand_on(b, j, q):
        pair_copy(b, j, q).start()
        write_part(b, j, q).start()

    singles = groups * (PARTS - 1)

    def single(s):
        return s // (PARTS - 1), 1 + lax.rem(s, PARTS - 1)

    def single_arrivals(s):
        u, q = single(s)
        for d in range(1, GROUP):
            j = peer(u, d)
            member_arrival(me, j, q).wait_recv()
            for i in range(1, chips):
                y_copy(i, j, q).start()
            hand_on(me, j, q)

    @pl.loop(0, singles)
    def _(s):
        u, q = single(s)
        j = peer(u, 0)

        @pl.when(jnp.logical_and(q == 1, u > 0))
        def _():
            first_arrival(0, u).wait_recv()

        compute(s, me, j, q)
        for i in range(1, chips):
            y_copy(i, j, q).start()
        for d in range(1, GROUP):
            member_copy(s, d, me, j, q).start()
        hand_on(me, j, q)

        @pl.when(s > 2)
        def _():
            single_arrivals(s - 3)

    for i in range(1, chips):
        @pl.loop(0, groups)
        def _(u):
            first_arrival(i, u).wait_recv()
            curve_arrival(i, u).wait_recv()

    doubles = groups * chips

    @pl.loop(0, doubles)
    def _(s):
        u = s // chips
        b = lax.rem(me + 2 * lax.rem(s, chips), bins)
        j = peer(u, 0)
        compute(singles + s, b, j, 0)
        for d in range(1, GROUP):
            member_copy(singles + s, d, b, j, 0).start()
        hand_on(b, j, 0)

        @pl.when(s < 3)
        def _():
            single_arrivals(singles - 3 + s)

    def second_copy(d, b, j):
        to = lax.rem(member + d, GROUP)
        return remote(lam_ref.at[b, j], lam_ref.at[b, j], bsend.at[b // 2, j // GROUP, d], brecv.at[b // 2, j], group * GROUP + to, me)

    @pl.loop(0, doubles)
    def _(s):
        b = lax.rem(me + 2 * lax.rem(s, chips), bins)
        for d in range(1, GROUP):
            second_copy(d, b, peer(s // chips, 0)).start()

    @pl.loop(0, doubles)
    def _(s):
        b = lax.rem(me + 2 * lax.rem(s, chips), bins)
        for d in range(1, GROUP):
            j = peer(s // chips, d)
            member_arrival(b, j, 0).wait_recv()
            hand_on(b, j, 0)

    @pl.loop(0, singles)
    def _(s):
        u, q = single(s)
        for d in range(GROUP):
            for i in range(1, chips):
                y_arrival(i, peer(u, d), q).wait_recv()
                hand_on(other_chip(i), peer(u, d), q)

    def lam_pair(b):
        return remote(lam_ref.at[b], lam_ref.at[b], lsend.at[b // 2], lrecv.at[b // 2], col, partner)

    for i in range(chips):
        b = other_chip(i)

        @pl.loop(0, groups)
        def _(u):
            for d in range(1, GROUP):
                second_copy(d, b, peer(u, d)).wait_recv()

        lam_pair(b).start()

    @pl.loop(0, cols)
    def _(j):
        for i in range(chips):
            b = other_chip(i)
            theirs = lax.rem(partner + 2 * i, bins)
            pair_chunk(theirs, j).wait_recv()
            write_chunk(theirs, j).start()

    for i in range(chips):
        lam_pair(other_chip(i)).wait()

    @pl.loop(0, cols)
    def _(j):
        for b in range(bins):
            write_chunk(b, j).wait()
        for i in range(chips):
            pair_chunk(other_chip(i), j).wait_send()
        for i in range(1, chips):
            for q in range(1, PARTS):
                y_copy(i, j, q).wait_send()

    @pl.loop(0, singles + doubles)
    def _(item):
        for d in range(1, GROUP):
            member_copy(item, d, me, col, 0).wait_send()

    @pl.loop(0, doubles)
    def _(s):
        b = lax.rem(me + 2 * lax.rem(s, chips), bins)
        for d in range(1, GROUP):
            second_copy(d, b, peer(s // chips, 0)).wait_send()

    @pl.loop(1, groups)
    def _(u):
        first_copy(0, u).wait_send()

    for i in range(1, chips):
        @pl.loop(0, groups)
        def _(u):
            first_copy(i, u).wait_send()
            curve_copy(i, u).wait_send()

    @pl.loop(1, cols)
    def _(i):
        table_copy(i).wait_send()


def per_device(slope, curvature, target_mean, target_var, table):
    cols = lax.axis_size("col")
    bins = lax.axis_size("bin")
    all_species, pts = table.shape
    rows = all_species // cols
    pad = rows
    total_pts = pts * cols
    per_shard = slope.shape[0]
    sub = per_shard // cols // LANES
    width = sub * LANES
    chips = bins // 2
    groups = cols // GROUP
    items = groups * (PARTS - 1 + chips)

    def blocks(a):
        return a.reshape(cols, sub, LANES)

    placed = table.reshape(cols, rows, pts)
    vmem = pl.BlockSpec(memory_space=pltpu.VMEM)
    hbm = pl.BlockSpec(memory_space=pltpu.HBM)
    dma = pltpu.SemaphoreType.DMA
    species_mean, lam = pl.pallas_call(
        functools.partial(kernel, cols, bins, total_pts, rows),
        out_shape=(
            jax.ShapeDtypeStruct((rows, per_shard * bins), jnp.float32),
            jax.ShapeDtypeStruct((bins, cols, sub, LANES), jnp.float32),
        ),
        in_specs=[hbm] * 4 + [vmem],
        out_specs=(pl.BlockSpec(memory_space=pl.ANY), vmem),
        scratch_shapes=[
            pltpu.VMEM((3, sub, LANES), jnp.float32),
            pltpu.VMEM((bins, cols, sub, LANES), jnp.float32),
            pltpu.VMEM((cols, GROUP, pad, pts), jnp.float32),
            pltpu.VMEM((2 * GROUP * pad + 16, total_pts), jnp.bfloat16),
            pltpu.VMEM((total_pts, LANES), jnp.float32),
            pltpu.VMEM((items, GROUP, rows, width // PARTS), jnp.float32),
            pltpu.VMEM((bins, cols, rows, width), jnp.float32),
            dma((4,)),
            dma((cols,)), dma((cols,)),
            dma((chips, groups)), dma((chips, cols)),
            dma((chips, groups)), dma((chips, cols)),
            dma((chips, groups, GROUP)), dma((chips, cols)),
            dma((chips,)), dma((chips,)),
            dma((items, GROUP)), dma((chips, cols, PARTS)),
            dma((chips, cols, PARTS)), dma((chips, cols, PARTS)),
            dma((chips, cols)), dma((chips, cols)),
            dma((bins, cols)),
        ],
        compiler_params=pltpu.CompilerParams(collective_id=0, has_side_effects=True, vmem_limit_bytes=40 << 20),
    )(*[
        pltpu.with_memory_space_constraint(a, pltpu.HBM)
        for a in (blocks(slope), blocks(curvature), blocks(target_mean), blocks(target_var))
    ], placed)
    return species_mean, lam.reshape(-1)


def solution(mesh):
    placed = (P("bin"), P("bin"), P("bin"), P("bin"), P(None, "col"))
    return jax.shard_map(
        per_device, mesh=mesh, in_specs=placed, out_specs=(P("col", None), P()), check_vma=False
    )
```
